32 devices in a mesh: dp: 2 (over x), sp: 16 (over y, z, core).
Axes of the slice: x: 2, y: 2, z: 4, core: 2. Of those that a mesh axis runs over, the one named last changes fastest.
Arguments:
- x: bfloat16 [16384, 2304], P(('dp', 'sp')), parts along dimension 0
- gain: bfloat16 [2304], replicated
- wq: bfloat16 [2304, 2048], replicated
- wk: bfloat16 [2304, 1024], replicated
- wv: bfloat16 [2304, 1024], replicated
- wo: bfloat16 [2048, 2304], replicated
Outputs:
- output: bfloat16 [16384, 2304], P(('dp', 'sp')), parts along dimension 0
There are 2 independent parts. The reference program is written for one: setup_inputs(seed, part) draws one part's arguments, and reference() takes and returns one part's arrays. A program takes and returns all parts, laid end to end along the dimension named above; an argument that names none is the same for every part.
All inputs are finite; a program needn't handle non-finite values.
Results may differ from the reference program's by a relative error of at most 0.012.
Values are sent between devices in bfloat16 or wider.
A program may use at most 2 GiB of HBM per device.

```python
import jax
import jax.numpy as jnp
from jax import lax

ROWS = 8192
D = 2304
HEADS = 8
KV_HEADS = 4
HEAD = 256
THETA = 10000


def setup_inputs(seed: int = 0, part: int = 0) -> dict:
    kx, kn, kq, kk, kv, ko = jax.random.split(jax.random.key(seed), 6)

    def weights(key, rows, columns):
        return jax.random.normal(key, (rows, columns), jnp.float32) * rows**-0.5

    drawn = {
        "x": jax.random.normal(jax.random.fold_in(kx, part), (ROWS, D), jnp.float32),
        "gain": 1 + 0.1 * jax.random.normal(kn, (D,), jnp.float32),
        "wq": 2 * weights(kq, D, HEADS * HEAD),
        "wk": 2 * weights(kk, D, KV_HEADS * HEAD),
        "wv": 4 * weights(kv, D, KV_HEADS * HEAD),
        "wo": weights(ko, HEADS * HEAD, D),
    }
    return {k: v.astype(jnp.bfloat16) for k, v in drawn.items()}


def normed(x, gain):
    wide = x.astype(jnp.float32)
    scale = lax.rsqrt(jnp.mean(wide * wide, -1, keepdims=True) + 1e-6)
    return (wide * scale * gain.astype(jnp.float32)).astype(jnp.bfloat16)


def turned(t, place, theta):
    half = t.shape[-1] // 2
    angle = place.astype(jnp.float32)[:, None] * theta ** (-jnp.arange(half, dtype=jnp.float32) / half)
    cos, sin = jnp.cos(angle)[:, None], jnp.sin(angle)[:, None]
    a, b = t[..., :half].astype(jnp.float32), t[..., half:].astype(jnp.float32)
    return jnp.concatenate([a * cos - b * sin, b * cos + a * sin], -1).astype(jnp.bfloat16)


def matmul(a, w):
    return jnp.dot(a, w, preferred_element_type=jnp.float32).astype(jnp.bfloat16)


def einsum(form, a, b):
    return jnp.einsum(form, a.astype(jnp.float32), b.astype(jnp.float32))


def attention(q, k, v):
    scores = einsum("tgsd,ugd->gstu", q, k) * q.shape[-1] ** -0.5
    token = jnp.arange(q.shape[0])
    scores = jnp.where(token[:, None] >= token, scores, -jnp.inf)
    weights = jax.nn.softmax(scores, -1).astype(jnp.bfloat16)
    return einsum("gstu,ugd->tgsd", weights, v).astype(jnp.bfloat16)


def reference(x, gain, wq, wk, wv, wo):
    a, place = normed(x, gain), jnp.arange(ROWS)
    q = turned(matmul(a, wq).reshape(ROWS, HEADS, HEAD), place, THETA).reshape(ROWS, KV_HEADS, -1, HEAD)
    k = turned(matmul(a, wk).reshape(ROWS, KV_HEADS, HEAD), place, THETA)
    v = matmul(a, wv).reshape(ROWS, KV_HEADS, HEAD)
    seen = attention(q, k, v).reshape(ROWS, HEADS * HEAD)
    return (x.astype(jnp.float32) + jnp.dot(seen, wo, preferred_element_type=jnp.float32)).astype(jnp.bfloat16)
```

```python
import functools

import jax
import jax.numpy as jnp
from jax import lax
from jax.experimental import pallas as pl
from jax.experimental.pallas import tpu as pltpu
from jax.sharding import PartitionSpec as P

NEG = -1e30
HIDDEN = 2 * NEG
LOG2E = 1.4426950408889634
HEAD = 256
THETA = 10000
KV = 4
HEADS = 8
DEVICES = 16
VMEM = 62 * 2**20


def _dot(a, b, ca, cb):
    return lax.dot_general(a, b, (((ca,), (cb,)), ((), ())), preferred_element_type=jnp.float32)


def _kernel(x_ref, gain_ref, cos_ref, sin_ref, wk, wv, wq, o_ref, a_s, wk_s, wv_s, wq_s, k_own, v_own, q_own, k_r, v_r, q_r, acc, top_s,
            o_s, w_sem, k_send, v_send, q_send, o_send, kf_send, vf_send, k_recv, v_recv, q_recv, o_recv):
    t = x_ref.shape[0]
    rows = min(t, 256)
    me, dp = lax.axis_index("sp"), lax.axis_index("dp")
    core = lax.rem(me, 2)
    z = lax.rem(lax.div(me, 2), 4)
    y = lax.div(me, 8)
    side = lax.div(z, 2)
    slot = y * 4 + lax.rem(z, 2) * 2 + core
    head = y * 2 + lax.rem(z, 2)
    inner = (z == 1) | (z == 2)

    def weights(i):
        if i < 2 * KV:
            src, dst = (wk, wk_s) if i % 2 == 0 else (wv, wv_s)
            n = i // 2
        else:
            src, dst, n = wq, wq_s, i - 2 * KV
        return pltpu.make_async_copy(src.at[:, n * HEAD : (n + 1) * HEAD], dst.at[n], w_sem.at[i])

    def arrived(ref, sem):
        pltpu.make_async_copy(ref, ref, sem).wait()

    for i in range(2 * KV + HEADS):
        weights(i).start()

    def norm(r, _):
        at = pl.ds(r * rows, rows)
        wide = x_ref[at, :].astype(jnp.float32)
        scale = lax.rsqrt(jnp.mean(wide * wide, -1, keepdims=True) + 1e-6)
        a_s[at, :] = (wide * scale * gain_ref[...].astype(jnp.float32)).astype(jnp.bfloat16)

    lax.fori_loop(0, t // rows, norm, None)

    def turned(r, at):
        half = HEAD // 2
        cos, sin = cos_ref[at, :], sin_ref[at, :]
        a, b = r[:, :half].astype(jnp.float32), r[:, half:].astype(jnp.float32)
        return jnp.concatenate([a * cos - b * sin, b * cos + a * sin], -1).astype(jnp.bfloat16)

    def project(n, w_s):
        for r in range(t // rows):
            at = pl.ds(r * rows, rows)
            yield at, _dot(a_s[at, :], w_s[n], 1, 0).astype(jnp.bfloat16)

    def deliver(src, dst, send, recv, to):
        @pl.when(to == me)
        def _():
            pltpu.make_async_copy(src, dst, recv).start()

        @pl.when(to != me)
        def _():
            pltpu.make_async_remote_copy(src_ref=src, dst_ref=dst, send_sem=send, recv_sem=recv, device_id=(dp, to),
                                         device_id_type=pl.DeviceIdType.MESH).start()

    def kv_to(n, s):
        return lax.div(n, 2) * 8 + s * 4 + lax.rem(n, 2) * 2 + core

    def q_to(n):
        return lax.div(n, 4) * 8 + side * 4 + lax.rem(lax.div(n, 2), 2) * 2 + lax.rem(n, 2)


    def send_kv(n, s):
        deliver(k_own.at[n], k_r.at[me], k_send.at[n * 2 + s], k_recv.at[me], kv_to(n, s))
        deliver(v_own.at[n], v_r.at[me], v_send.at[n * 2 + s], v_recv.at[me], kv_to(n, s))

    def over(n):
        @pl.when((side == 0) | (me < 12))
        def _():
            send_kv(n, 1 - side)

    def make_kv(n, _):
        arrived(wk_s.at[n], w_sem.at[n * 2])
        for at, r in project(n, wk_s):
            k_own[n, at, :] = turned(r, at)
        arrived(wv_s.at[n], w_sem.at[n * 2 + 1])
        for at, r in project(n, wv_s):
            v_own[n, :, at] = r.T
        send_kv(n, side)

        @pl.when(inner)
        def _():
            over(n)

    lax.fori_loop(0, KV, make_kv, None)

    def make_q(n, _):
        arrived(wq_s.at[n], w_sem.at[2 * KV + n])
        for at, r in project(n, wq_s):
            q_own[n, at, :] = turned(r, at)
        deliver(q_own.at[n], q_r.at[slot], q_send.at[n], q_recv.at[slot], q_to(n))

    lax.fori_loop(0, HEADS, make_q, None)

    @pl.when(jnp.logical_not(inner))
    def _():
        lax.fori_loop(0, KV, lambda n, _: over(n), None)

    for i in range(8):
        top_s[i] = jnp.full((1, t), NEG, jnp.float32)
        acc[i] = jnp.zeros((HEAD + 8, t), jnp.float32)
    lax.fori_loop(0, 8, lambda i, _: arrived(q_r.at[i], q_recv.at[i]), None)

    e = HEAD**-0.5 * LOG2E
    ones = jnp.ones((8, t), jnp.bfloat16)

    def block(kb, g, masked):
        at = [g * 4 + n for n in range(4)]
        scores = [_dot(k_r[kb], q_r[i], 1, 1) for i in at]
        if masked:
            gap = lax.broadcasted_iota(jnp.int32, (t, t), 1) - lax.broadcasted_iota(jnp.int32, (t, t), 0)
            first = (g * 8 + side * 4 - kb) * t
            scores = [jnp.where(gap >= -(first + n * t), s, HIDDEN) for n, s in enumerate(scores)]
        weights, keeps = [], []
        for i, s in zip(at, scores):
            old = top_s[i]
            top = jnp.maximum(old, s.max(axis=0, keepdims=True))
            top_s[i] = top
            weights.append(jnp.exp2((s - top) * e).astype(jnp.bfloat16))
            keeps.append(jnp.exp2((old - top) * e))
        values = jnp.concatenate([v_r[kb], ones], axis=0)
        for i, p, keep in zip(at, weights, keeps):
            acc[i] = acc[i] * keep + _dot(values, p, 1, 0)

    def attend(kb):
        def row(g, _):
            first = g * 8 + side * 4

            @pl.when(kb < first)
            def _():
                block(kb, g, False)

            @pl.when((kb >= first) & (kb < first + 4))
            def _():
                block(kb, g, True)

        lax.fori_loop(0, 2, row, None)

    def chip(m, _):
        own_side = m < 4
        mm = lax.rem(m, 4)
        far, row = lax.div(mm, 2), lax.rem(mm, 2)
        zz = jnp.where(side == 1, 1 - far, far)
        base = jnp.where(own_side, lax.div(mm, 2) * 8 + side * 4 + lax.rem(mm, 2) * 2, row * 8 + (1 - side) * 4 + zz * 2)

        @pl.when((side == 1) | (base < 12))
        def _():
            mine, other = base + core, base + 1 - core
            arrived(k_r.at[mine], k_recv.at[mine])
            arrived(v_r.at[mine], v_recv.at[mine])
            sibling = me + 1 - 2 * core
            for ref, send, recv in ((k_r, kf_send, k_recv), (v_r, vf_send, v_recv)):
                pltpu.make_async_remote_copy(src_ref=ref.at[mine], dst_ref=ref.at[mine], send_sem=send.at[m], recv_sem=recv.at[mine],
                                             device_id=(dp, sibling), device_id_type=pl.DeviceIdType.MESH).start()
            attend(mine)
            arrived(k_r.at[other], k_recv.at[other])
            arrived(v_r.at[other], v_recv.at[other])
            attend(other)

    lax.fori_loop(0, 8, chip, None)

    def finish(i, _):
        o_s[i] = (acc[i, :HEAD, :] * (1 / acc[i, HEAD : HEAD + 1, :])).T.astype(jnp.bfloat16)
        to = lax.div(i, 4) * 8 + side * 4 + lax.rem(i, 4)
        j = head * 2 + core
        deliver(o_s.at[i], o_ref.at[j], o_send.at[i], o_recv.at[j], to)

    lax.fori_loop(0, 8, finish, None)

    def left(ref, sem):
        pltpu.make_async_copy(ref, ref, sem).wait()

    def ends(n, _):
        for s in range(2):
            @pl.when((kv_to(n, s) != me) & ((s == side) | (side == 0) | (me < 12)))
            def _():
                left(k_own.at[n], k_send.at[n * 2 + s])
                left(v_own.at[n], v_send.at[n * 2 + s])

    lax.fori_loop(0, KV, ends, None)

    def q_ends(n, _):
        @pl.when(q_to(n) != me)
        def _():
            left(q_own.at[n], q_send.at[n])

        @pl.when(n != slot)
        def _():
            left(o_s.at[n], o_send.at[n])

        arrived(o_s.at[n], o_recv.at[n])

    lax.fori_loop(0, HEADS, q_ends, None)

    def f_ends(m, _):
        mm = lax.rem(m, 4)

        @pl.when((side == 1) | (m < 4) | (lax.rem(mm, 2) == 0))
        def _():
            left(k_r.at[0], kf_send.at[m])
            left(v_r.at[0], vf_send.at[m])

    lax.fori_loop(0, 8, f_ends, None)


def solution(mesh):
    def step(x, gain, wq, wk, wv, wo):
        t, d = x.shape
        first = lax.axis_index("sp") * t
        half = HEAD // 2
        angle = (first + jnp.arange(t)).astype(jnp.float32)[:, None] * THETA ** (-jnp.arange(half, dtype=jnp.float32) / half)
        bf, f32, dma = jnp.bfloat16, jnp.float32, pltpu.SemaphoreType.DMA
        vmem, hbm = pl.BlockSpec(memory_space=pltpu.VMEM), pl.BlockSpec(memory_space=pl.ANY)
        o = pl.pallas_call(
            _kernel,
            in_specs=[vmem] * 4 + [hbm] * 3,
            out_specs=hbm,
            out_shape=jax.ShapeDtypeStruct((HEADS, t, HEAD), bf),
            scratch_shapes=[
                pltpu.VMEM((t, d), bf),
                pltpu.VMEM((KV, d, HEAD), bf), pltpu.VMEM((KV, d, HEAD), bf), pltpu.VMEM((HEADS, d, HEAD), bf),
                pltpu.VMEM((KV, t, HEAD), bf), pltpu.VMEM((KV, HEAD, t), bf), pltpu.VMEM((HEADS, t, HEAD), bf),
                pltpu.VMEM((DEVICES, t, HEAD), bf), pltpu.VMEM((DEVICES, HEAD, t), bf), pltpu.VMEM((8, t, HEAD), bf),
                pltpu.VMEM((8, HEAD + 8, t), f32), pltpu.VMEM((8, 1, t), f32), pltpu.VMEM((8, t, HEAD), bf),
                dma((2 * KV + HEADS,)), dma((2 * KV,)), dma((2 * KV,)), dma((HEADS,)), dma((8,)), dma((8,)), dma((8,)),
                dma((DEVICES,)), dma((DEVICES,)), dma((8,)), dma((HEADS,)),
            ],
            compiler_params=pltpu.CompilerParams(has_side_effects=True, vmem_limit_bytes=VMEM),
            name="attention",
        )(x, gain[None], jnp.cos(angle), jnp.sin(angle), wk, wv, wq)
        y = jnp.einsum("htd,hdn->tn", o, wo.reshape(HEADS, HEAD, d), preferred_element_type=f32)
        return (x.astype(f32) + y).astype(bf)

    tokens, whole = P(("dp", "sp"), None), P(None, None)
    return jax.shard_map(
        step,
        mesh=mesh,
        in_specs=(tokens, P(None), whole, whole, whole, whole),
        out_specs=tokens,
        check_vma=False,
    )
```

```python
import functools

import jax
import jax.numpy as jnp
from jax import lax
from jax.experimental import pallas as pl
from jax.experimental.pallas import tpu as pltpu
from jax.sharding import PartitionSpec as P

NEG = -1e30
HIDDEN = 2 * NEG
LOG2E = 1.4426950408889634
HEAD = 256
THETA = 10000
KV = 4
HEADS = 8
DEVICES = 16
VMEM = 63 * 2**20


def _dot(a, b, ca, cb):
    return lax.dot_general(a, b, (((ca,), (cb,)), ((), ())), preferred_element_type=jnp.float32)


def _kernel(x_ref, gain_ref, cos_ref, sin_ref, wk, wv, wq, o_ref, a_s, wk_s, wv_s, wq_s, k_own, v_own, q_own, k_r, v_r, q_r, acc, top_s,
            o_s, w_sem, own_send, q_send, o_send, pass_send, k_recv, v_recv, q_recv, o_recv):
    t = x_ref.shape[0]
    rows = min(t, 256)
    me, dp = lax.axis_index("sp"), lax.axis_index("dp")
    core = lax.rem(me, 2)
    z = lax.rem(lax.div(me, 2), 4)
    y = lax.div(me, 8)
    side = lax.div(z, 2)
    inner = (z == 1) | (z == 2)

    def at_chip(r, column, c):
        return r * 8 + column * 2 + c

    def weights(i):
        if i < 2 * KV:
            src, dst = (wk, wk_s) if i % 2 == 0 else (wv, wv_s)
            n = i // 2
        else:
            src, dst, n = wq, wq_s, i - 2 * KV
        return pltpu.make_async_copy(src.at[:, n * HEAD : (n + 1) * HEAD], dst.at[n], w_sem.at[i])

    def arrived(ref, sem):
        pltpu.make_async_copy(ref, ref, sem).wait()

    for i in range(2 * KV + HEADS):
        weights(i).start()

    def norm(r, _):
        at = pl.ds(r * rows, rows)
        wide = x_ref[at, :].astype(jnp.float32)
        scale = lax.rsqrt(jnp.mean(wide * wide, -1, keepdims=True) + 1e-6)
        a_s[at, :] = (wide * scale * gain_ref[...].astype(jnp.float32)).astype(jnp.bfloat16)

    lax.fori_loop(0, t // rows, norm, None)

    def turned(r, at):
        half = HEAD // 2
        cos, sin = cos_ref[at, :], sin_ref[at, :]
        a, b = r[:, :half].astype(jnp.float32), r[:, half:].astype(jnp.float32)
        return jnp.concatenate([a * cos - b * sin, b * cos + a * sin], -1).astype(jnp.bfloat16)

    def project(n, w_s):
        for r in range(t // rows):
            at = pl.ds(r * rows, rows)
            yield at, _dot(a_s[at, :], w_s[n], 1, 0).astype(jnp.bfloat16)

    def remote(src, dst, send, recv, to):
        return pltpu.make_async_remote_copy(src_ref=src, dst_ref=dst, send_sem=send, recv_sem=recv, device_id=(dp, to),
                                            device_id_type=pl.DeviceIdType.MESH)

    def deliver(src, dst, send, recv, to):
        @pl.when(to == me)
        def _():
            pltpu.make_async_copy(src, dst, recv).start()

        @pl.when(to != me)
        def _():
            remote(src, dst, send, recv, to).start()

    middle = 1 + side
    block_here = y * 4 + z

    def entry(n):
        return at_chip(lax.rem(n, 2), jnp.where(n < 2, middle, z), core)

    def onward(kind, b):
        zb, early = lax.rem(b, 4), b < 4
        east = jnp.where(kind == 0, (z == 1) & (zb < 2), (z < 3) & (zb <= z))
        west = early & jnp.where(kind == 0, (z == 2) & (zb >= 2), (z > 0) & (zb >= z))
        return (east, me + 2), (west, me - 2)

    def both(ks, vs, kind, at, sends, to, start):
        for i, (src, dst, recv) in enumerate(((ks, k_r, k_recv), (vs, v_r, v_recv))):
            copy = remote(src, dst.at[kind, at], sends(i), recv.at[kind, at], to)
            copy.start() if start else copy.wait_send()

    def own_kv(n, start):
        kind, to = lax.div(n, 2), entry(n)
        ks, vs = k_own.at[n], v_own.at[n]

        @pl.when(to != me)
        def _():
            both(ks, vs, kind, me, lambda i: own_send.at[i, n, 0], to, start)

        @pl.when(to == me)
        def _():
            if start:
                pltpu.make_async_copy(ks, k_r.at[kind, me], k_recv.at[kind, me]).start()
                pltpu.make_async_copy(vs, v_r.at[kind, me], v_recv.at[kind, me]).start()
            for d, (ok, on) in enumerate(onward(kind, block_here)):
                @pl.when(ok)
                def _():
                    both(ks, vs, kind, me, lambda i: own_send.at[i, n, 1 + d], on, start)

    def q_to(n):
        kind = lax.div(n, 4)
        return at_chip(lax.rem(lax.div(n, 2), 2), jnp.where(kind == 0, middle, z), lax.rem(n, 2))

    def q_place(n):
        return jnp.where(n < 4, y * 4 + (z - 2 * side) * 2 + core, 8 + y * 2 + core)

    def make_kv(n, _):
        arrived(wk_s.at[n], w_sem.at[n * 2])
        for at, r in project(n, wk_s):
            k_own[n, at, :] = turned(r, at)
        arrived(wv_s.at[n], w_sem.at[n * 2 + 1])
        for at, r in project(n, wv_s):
            v_own[n, :, at] = r.T
        own_kv(n, True)

    lax.fori_loop(0, KV, make_kv, None)

    def make_q(n, _):
        arrived(wq_s.at[n], w_sem.at[2 * KV + n])
        for at, r in project(n, wq_s):
            q_own[n, at, :] = turned(r, at)
        i = q_place(n)
        deliver(q_own.at[n], q_r.at[i], q_send.at[n], q_recv.at[i], q_to(n))

    lax.fori_loop(0, HEADS, make_q, None)

    def clear(i, _):
        top_s[i] = jnp.full((1, t), NEG, jnp.float32)
        acc[i] = jnp.zeros((HEAD + 8, t), jnp.float32)

    lowest = jnp.where(inner, 0, 8)
    lax.fori_loop(lowest, 12, clear, None)
    lax.fori_loop(lowest, 12, lambda i, _: arrived(q_r.at[i], q_recv.at[i]), None)

    e = HEAD**-0.5 * LOG2E
    ones = jnp.ones((8, t), jnp.bfloat16)

    def block(kind, kb, slots, places, masked):
        scores = [_dot(k_r[kind, kb], q_r[i], 1, 1) for i in slots]
        if masked:
            gap = lax.broadcasted_iota(jnp.int32, (t, t), 1) - lax.broadcasted_iota(jnp.int32, (t, t), 0)
            scores = [jnp.where(gap >= (kb - p) * t, s, HIDDEN) for p, s in zip(places, scores)]
        weights, keeps = [], []
        for i, s in zip(slots, scores):
            old = top_s[i]
            top = jnp.maximum(old, s.max(axis=0, keepdims=True))
            top_s[i] = top
            weights.append(jnp.exp2((s - top) * e).astype(jnp.bfloat16))
            keeps.append(jnp.exp2((old - top) * e))
        values = jnp.concatenate([v_r[kind, kb], ones], axis=0)
        for i, p, keep in zip(slots, weights, keeps):
            acc[i] = acc[i] * keep + _dot(values, p, 1, 0)

    def attend(kind, kb):
        def row(g, _):
            first = g * 8 + side * 4
            slots, places = [g * 4 + n for n in range(4)], [first + n for n in range(4)]

            @pl.when(kb < first)
            def _():
                block(0, kb, slots, places, False)

            @pl.when((kb >= first) & (kb < first + 4))
            def _():
                block(0, kb, slots, places, True)

        @pl.when(kind == 0)
        def _():
            lax.fori_loop(0, 2, row, None)

        first = z * 2
        slots, places = [8, 9, 10, 11], [first, first + 1, first + 8, first + 9]

        @pl.when((kind == 1) & (kb < first))
        def _():
            block(1, kb, slots, places, False)

        @pl.when((kind == 1) & (kb >= first) & (kb < first + 2))
        def _():
            block(1, kb, slots, places, True)

        @pl.when((kind == 1) & (kb >= first + 2) & (kb < first + 8))
        def _():
            block(1, kb, slots[2:], places[2:], False)

        @pl.when((kind == 1) & (kb >= first + 8))
        def _():
            block(1, kb, slots[2:], places[2:], True)

    sibling = me + 1 - 2 * core

    def decode(n):
        s = jnp.where(n < 8, side, 1 - side)
        m = lax.rem(n, 8)
        row, kind, o = lax.div(m, 4), lax.rem(lax.div(m, 2), 2), lax.rem(m, 2)
        b = row * 4 + jnp.where(o == 0, 1 + s, 3 * s)
        return kind, b, jnp.where(kind == 0, inner & ((side == 1) | (b < 6)), b <= z + 4)

    def passed(n, kind, b, start):
        mine = b * 2 + core
        ks, vs = k_r.at[kind, mine], v_r.at[kind, mine]
        both(ks, vs, kind, mine, lambda i: pass_send.at[i, n, 2], sibling, start)

        @pl.when(b != block_here)
        def _():
            for d, (ok, on) in enumerate(onward(kind, b)):
                @pl.when(ok)
                def _():
                    both(ks, vs, kind, mine, lambda i: pass_send.at[i, n, d], on, start)

    def o_to(i):
        return jnp.where(i < 8, lax.div(i, 4) * 8 + side * 4 + lax.rem(i, 4), lax.div(i - 8, 2) * 8 + z * 2 + lax.rem(i, 2))

    def finish(i, _):
        o_s[i] = (acc[i, :HEAD, :] * (1 / acc[i, HEAD : HEAD + 1, :])).T.astype(jnp.bfloat16)
        j = (y + jnp.where(i < 8, 0, 2)) * 2 + core
        deliver(o_s.at[i], o_ref.at[j], o_send.at[i], o_recv.at[j], o_to(i))

    def step(n, _):
        kind, b, needed = decode(n)

        @pl.when(needed)
        def _():
            mine, other = b * 2 + core, b * 2 + 1 - core
            arrived(k_r.at[kind, mine], k_recv.at[kind, mine])
            arrived(v_r.at[kind, mine], v_recv.at[kind, mine])
            passed(n, kind, b, True)
            attend(kind, mine)
            arrived(k_r.at[kind, other], k_recv.at[kind, other])
            arrived(v_r.at[kind, other], v_recv.at[kind, other])
            attend(kind, other)

        @pl.when((n >= 8) & (lax.rem(n, 2) == 1) & (inner | (kind == 1)))
        def _():
            row = jnp.where(n < 12, 0, 1)
            first = jnp.where(kind == 0, row * 4, 8 + row * 2)
            lax.fori_loop(first, first + jnp.where(kind == 0, 4, 2), finish, None)

    lax.fori_loop(0, 16, step, None)

    lax.fori_loop(0, KV, lambda n, _: own_kv(n, False), None)

    def q_ends(n, _):
        @pl.when(q_to(n) != me)
        def _():
            arrived(q_own.at[n], q_send.at[n])

        arrived(o_s.at[n], o_recv.at[n])

    lax.fori_loop(0, HEADS, q_ends, None)

    def o_ends(i, _):
        @pl.when(o_to(i) != me)
        def _():
            arrived(o_s.at[i], o_send.at[i])

    lax.fori_loop(lowest, 12, o_ends, None)

    def pass_ends(n, _):
        kind, b, needed = decode(n)

        @pl.when(needed)
        def _():
            passed(n, kind, b, False)

    lax.fori_loop(0, 16, pass_ends, None)


def solution(mesh):
    def step(x, gain, wq, wk, wv, wo):
        t, d = x.shape
        first = lax.axis_index("sp") * t
        half = HEAD // 2
        angle = (first + jnp.arange(t)).astype(jnp.float32)[:, None] * THETA ** (-jnp.arange(half, dtype=jnp.float32) / half)
        bf, f32, dma = jnp.bfloat16, jnp.float32, pltpu.SemaphoreType.DMA
        vmem, hbm = pl.BlockSpec(memory_space=pltpu.VMEM), pl.BlockSpec(memory_space=pl.ANY)
        o = pl.pallas_call(
            _kernel,
            in_specs=[vmem] * 4 + [hbm] * 3,
            out_specs=hbm,
            out_shape=jax.ShapeDtypeStruct((HEADS, t, HEAD), bf),
            scratch_shapes=[
                pltpu.VMEM((t, d), bf),
                pltpu.VMEM((KV, d, HEAD), bf), pltpu.VMEM((KV, d, HEAD), bf), pltpu.VMEM((HEADS, d, HEAD), bf),
                pltpu.VMEM((KV, t, HEAD), bf), pltpu.VMEM((KV, HEAD, t), bf), pltpu.VMEM((HEADS, t, HEAD), bf),
                pltpu.VMEM((2, DEVICES, t, HEAD), bf), pltpu.VMEM((2, DEVICES, HEAD, t), bf), pltpu.VMEM((12, t, HEAD), bf),
                pltpu.VMEM((12, HEAD + 8, t), f32), pltpu.VMEM((12, 1, t), f32), pltpu.VMEM((12, t, HEAD), bf),
                dma((2 * KV + HEADS,)), dma((2, KV, 3)), dma((HEADS,)), dma((12,)), dma((2, 16, 3)),
                dma((2, DEVICES)), dma((2, DEVICES)), dma((12,)), dma((HEADS,)),
            ],
            compiler_params=pltpu.CompilerParams(has_side_effects=True, vmem_limit_bytes=VMEM),
            name="attention",
        )(x, gain[None], jnp.cos(angle), jnp.sin(angle), wk, wv, wq)
        y = jnp.einsum("htd,hdn->tn", o, wo.reshape(HEADS, HEAD, d), preferred_element_type=f32)
        return (x.astype(f32) + y).astype(bf)

    tokens, whole = P(("dp", "sp"), None), P(None, None)
    return jax.shard_map(
        step,
        mesh=mesh,
        in_specs=(tokens, P(None), whole, whole, whole, whole),
        out_specs=tokens,
        check_vma=False,
    )
```

```python
import functools

import jax
import jax.numpy as jnp
import numpy as np
from jax import lax
from jax.experimental import pallas as pl
from jax.experimental.pallas import tpu as pltpu
from jax.sharding import PartitionSpec as P

NEG = -1e30
HIDDEN = 2 * NEG
LOG2E = 1.4426950408889634
HEAD = 256
THETA = 10000
KV = 4
HEADS = 8
DEVICES = 16
VMEM = 63 * 2**20
EARLY = 2


def _dot(a, b, ca, cb):
    return lax.dot_general(a, b, (((ca,), (cb,)), ((), ())), preferred_element_type=jnp.float32)


def _kernel(x_ref, gain_ref, turn_ref, start_ref, wk, wv, wq, wo, y_ref, a_s, cos_s, sin_s, wk_s, wv_s, wq_s, k_own, v_own, q_own, k_r, v_r,
            q_r, acc, top_s, o_s, o_r, y_s, w_sem, wo_sem, k_send, v_send, q_send, o_send, kf_send, vf_send, k_recv, v_recv, q_recv, o_recv):
    t, d = x_ref.shape
    width = HEADS * HEAD
    rows = min(t, 256)
    me, dp = lax.axis_index("sp"), lax.axis_index("dp")
    core = lax.rem(me, 2)
    z = lax.rem(lax.div(me, 2), 4)
    y = lax.div(me, 8)
    side = lax.div(z, 2)
    slot = y * 4 + lax.rem(z, 2) * 2 + core
    head = y * 2 + lax.rem(z, 2)
    inner = (z == 1) | (z == 2)

    def weights(i):
        if i < 2 * KV:
            src, dst = (wk, wk_s) if i % 2 == 0 else (wv, wv_s)
            n = i // 2
        else:
            src, n = wq, i - 2 * KV
            dst = wq_s.at[n * d : (n + 1) * d, :]
        return pltpu.make_async_copy(src.at[:, n * HEAD : (n + 1) * HEAD], dst.at[n] if i < 2 * KV else dst, w_sem.at[i])

    def arrived(ref, sem):
        pltpu.make_async_copy(ref, ref, sem).wait()

    for i in range(2 * KV + HEADS):
        weights(i).start()

    def norm(r, _):
        at = pl.ds(r * rows, rows)
        wide = x_ref[at, :].astype(jnp.float32)
        scale = lax.rsqrt(jnp.mean(wide * wide, -1, keepdims=True) + 1e-6)
        a_s[at, :] = (wide * scale * gain_ref[...].astype(jnp.float32)).astype(jnp.bfloat16)

    lax.fori_loop(0, t // rows, norm, None)

    cos_a, sin_a = start_ref[me][:1, : HEAD // 2], start_ref[me][:1, HEAD // 2 :]
    cos_b, sin_b = turn_ref[:, : HEAD // 2], turn_ref[:, HEAD // 2 :]
    cos_s[...] = cos_a * cos_b - sin_a * sin_b
    sin_s[...] = sin_a * cos_b + cos_a * sin_b

    def turned(r, at):
        half = HEAD // 2
        cos, sin = cos_s[at, :], sin_s[at, :]
        a, b = r[:, :half].astype(jnp.float32), r[:, half:].astype(jnp.float32)
        return jnp.concatenate([a * cos - b * sin, b * cos + a * sin], -1).astype(jnp.bfloat16)

    def project(w):
        for r in range(t // rows):
            at = pl.ds(r * rows, rows)
            yield at, _dot(a_s[at, :], w, 1, 0).astype(jnp.bfloat16)

    def deliver(src, dst, send, recv, to):
        @pl.when(to == me)
        def _():
            pltpu.make_async_copy(src, dst, recv).start()

        @pl.when(to != me)
        def _():
            pltpu.make_async_remote_copy(src_ref=src, dst_ref=dst, send_sem=send, recv_sem=recv, device_id=(dp, to),
                                         device_id_type=pl.DeviceIdType.MESH).start()

    def kv_to(n, s):
        return lax.div(n, 2) * 8 + s * 4 + lax.rem(n, 2) * 2 + core

    def q_to(n):
        return lax.div(n, 4) * 8 + side * 4 + lax.rem(lax.div(n, 2), 2) * 2 + lax.rem(n, 2)


    def send_kv(n, s):
        deliver(k_own.at[n], k_r.at[me], k_send.at[n * 2 + s], k_recv.at[me], kv_to(n, s))
        deliver(v_own.at[n], v_r.at[me], v_send.at[n * 2 + s], v_recv.at[me], kv_to(n, s))

    def over(n):
        @pl.when((side == 0) | (me < 12))
        def _():
            send_kv(n, 1 - side)

    def make_kv(n, _):
        arrived(wk_s.at[n], w_sem.at[n * 2])
        for at, r in project(wk_s[n]):
            k_own[n, at, :] = turned(r, at)
        arrived(wv_s.at[n], w_sem.at[n * 2 + 1])
        for at, r in project(wv_s[n]):
            v_own[n, :, at] = r.T

        @pl.when(n < EARLY)
        def _():
            send_kv(n, side)

        @pl.when(inner)
        def _():
            over(n)

    lax.fori_loop(0, KV, make_kv, None)

    def make_q(n, _):
        arrived(wk_s.at[0], w_sem.at[2 * KV + n])
        for at, r in project(wq_s[pl.ds(pl.multiple_of(n * d, 256), d), :]):
            q_own[n, at, :] = turned(r, at)
        deliver(q_own.at[n], q_r.at[slot], q_send.at[n], q_recv.at[slot], q_to(n))

    lax.fori_loop(0, HEADS, make_q, None)
    lax.fori_loop(EARLY, KV, lambda n, _: send_kv(n, side), None)

    def out_weights(n):
        at = pl.ds(n * HEAD, HEAD) if isinstance(n, int) else pl.ds(pl.multiple_of(n * HEAD, HEAD), HEAD)
        to = pl.ds(pl.multiple_of(n * width, width), width)
        return pltpu.make_async_copy(wo.at[:, at], wq_s.at[to, :], wo_sem.at[n])

    lax.fori_loop(0, d // HEAD, lambda n, _: out_weights(n).start(), None)

    @pl.when(jnp.logical_not(inner))
    def _():
        lax.fori_loop(0, KV, lambda n, _: over(n), None)

    for i in range(8):
        top_s[i] = jnp.full((1, t), NEG, jnp.float32)
        acc[i] = jnp.zeros((HEAD + 8, t), jnp.float32)
    lax.fori_loop(0, 8, lambda i, _: arrived(q_r.at[i], q_recv.at[i]), None)

    e = HEAD**-0.5 * LOG2E
    ones = jnp.ones((8, t), jnp.bfloat16)

    def block(kb, g, masked):
        at = [g * 4 + n for n in range(4)]
        scores = [_dot(k_r[kb], q_r[i], 1, 1) for i in at]
        if masked:
            gap = lax.broadcasted_iota(jnp.int32, (t, t), 1) - lax.broadcasted_iota(jnp.int32, (t, t), 0)
            first = (g * 8 + side * 4 - kb) * t
            scores = [jnp.where(gap >= -(first + n * t), s, HIDDEN) for n, s in enumerate(scores)]
        weights, keeps = [], []
        for i, s in zip(at, scores):
            old = top_s[i]
            top = jnp.maximum(old, s.max(axis=0, keepdims=True))
            top_s[i] = top
            weights.append(jnp.exp2((s - top) * e).astype(jnp.bfloat16))
            keeps.append(jnp.exp2((old - top) * e))
        values = jnp.concatenate([v_r[kb], ones], axis=0)
        for i, p, keep in zip(at, weights, keeps):
            acc[i] = acc[i] * keep + _dot(values, p, 1, 0)

    def attend(kb):
        def row(g, _):
            first = g * 8 + side * 4

            @pl.when(kb < first)
            def _():
                block(kb, g, False)

            @pl.when((kb >= first) & (kb < first + 4))
            def _():
                block(kb, g, True)

        lax.fori_loop(0, 2, row, None)

    def finish(n, _):
        m = lax.rem(n, 4)
        i = n - m + lax.rem(m + 2 - 2 * lax.rem(z, 2), 4)
        o_s[i] = (acc[i, :HEAD, :] * (1 / acc[i, HEAD : HEAD + 1, :])).T.astype(jnp.bfloat16)
        to = lax.div(i, 4) * 8 + side * 4 + lax.rem(i, 4)
        j = head * 2 + core
        deliver(o_s.at[i], o_r.at[j], o_send.at[i], o_recv.at[j], to)

    def chip(m, _):
        own_side = m < 4
        mm = lax.rem(m, 4)
        far, row = lax.div(mm, 2), lax.rem(mm, 2)
        zz = jnp.where(side == 1, 1 - far, far)
        base = jnp.where(own_side, lax.div(mm, 2) * 8 + side * 4 + lax.rem(mm, 2) * 2, row * 8 + (1 - side) * 4 + zz * 2)

        @pl.when((side == 1) | (base < 12))
        def _():
            mine, other = base + core, base + 1 - core
            arrived(k_r.at[mine], k_recv.at[mine])
            arrived(v_r.at[mine], v_recv.at[mine])
            sibling = me + 1 - 2 * core
            for ref, send, recv in ((k_r, kf_send, k_recv), (v_r, vf_send, v_recv)):
                pltpu.make_async_remote_copy(src_ref=ref.at[mine], dst_ref=ref.at[mine], send_sem=send.at[m], recv_sem=recv.at[mine],
                                             device_id=(dp, sibling), device_id_type=pl.DeviceIdType.MESH).start()
            attend(mine)
            arrived(k_r.at[other], k_recv.at[other])
            arrived(v_r.at[other], v_recv.at[other])
            attend(other)

        done = m == jnp.where(side == 0, 1, 6)

        @pl.when(done | (m == 7))
        def _():
            at = jnp.where(done, 0, 4)
            lax.fori_loop(at, at + 4, finish, None)

    lax.fori_loop(0, 8, chip, None)

    for i in range(4):
        j = (lax.rem(y + i % 2, 2) * 2 + lax.rem(lax.rem(z, 2) + i // 2, 2)) * 2
        for n in range(2):
            arrived(o_s.at[0], o_recv.at[j + n])

        def columns(n, _):
            at = pl.ds(pl.multiple_of(n * HEAD, HEAD), HEAD)
            if i == 0:
                out_weights(n).wait()
            w = wq_s[pl.ds(pl.multiple_of(n * width + j * HEAD, 2 * HEAD), 2 * HEAD), :]
            part = _dot(o_r[j], w[:HEAD], 1, 0) + _dot(o_r[j + 1], w[HEAD:], 1, 0)
            part += x_ref[:, at].astype(jnp.float32) if i == 0 else y_s[:, at]
            if i < 3:
                y_s[:, at] = part
            else:
                y_ref[:, at] = part.astype(jnp.bfloat16)

        lax.fori_loop(0, d // HEAD, columns, None)

    def left(ref, sem):
        pltpu.make_async_copy(ref, ref, sem).wait()

    def ends(n, _):
        for s in range(2):
            @pl.when((kv_to(n, s) != me) & ((s == side) | (side == 0) | (me < 12)))
            def _():
                left(k_own.at[n], k_send.at[n * 2 + s])
                left(v_own.at[n], v_send.at[n * 2 + s])

    lax.fori_loop(0, KV, ends, None)

    def q_ends(n, _):
        @pl.when(q_to(n) != me)
        def _():
            left(q_own.at[n], q_send.at[n])

        @pl.when(n != slot)
        def _():
            left(o_s.at[n], o_send.at[n])


    lax.fori_loop(0, HEADS, q_ends, None)

    def f_ends(m, _):
        mm = lax.rem(m, 4)

        @pl.when((side == 1) | (m < 4) | (lax.rem(mm, 2) == 0))
        def _():
            left(k_r.at[0], kf_send.at[m])
            left(v_r.at[0], vf_send.at[m])

    lax.fori_loop(0, 8, f_ends, None)


def solution(mesh):
    def step(x, gain, wq, wk, wv, wo):
        t, d = x.shape
        half = HEAD // 2
        power = float(THETA) ** (-np.arange(half) / half)
        turns = [np.concatenate([np.cos(a), np.sin(a)], 1).astype(np.float32) for a in (np.arange(t)[:, None] * power,
                                                                                      np.arange(DEVICES)[:, None] * t * power)]
        turns[1] = np.repeat(turns[1][:, None], 8, 1)
        bf, f32, dma = jnp.bfloat16, jnp.float32, pltpu.SemaphoreType.DMA
        vmem, hbm = pl.BlockSpec(memory_space=pltpu.VMEM), pl.BlockSpec(memory_space=pl.ANY)
        return pl.pallas_call(
            _kernel,
            in_specs=[vmem] * 4 + [hbm] * 4,
            out_specs=vmem,
            out_shape=jax.ShapeDtypeStruct((t, d), bf),
            scratch_shapes=[
                pltpu.VMEM((t, d), bf), pltpu.VMEM((t, half), f32), pltpu.VMEM((t, half), f32),
                pltpu.VMEM((KV, d, HEAD), bf), pltpu.VMEM((KV, d, HEAD), bf), pltpu.VMEM((HEADS * d, HEAD), bf),
                pltpu.VMEM((KV, t, HEAD), bf), pltpu.VMEM((KV, HEAD, t), bf), pltpu.VMEM((HEADS, t, HEAD), bf),
                pltpu.VMEM((DEVICES, t, HEAD), bf), pltpu.VMEM((DEVICES, HEAD, t), bf), pltpu.VMEM((8, t, HEAD), bf),
                pltpu.VMEM((8, HEAD + 8, t), f32), pltpu.VMEM((8, 1, t), f32), pltpu.VMEM((8, t, HEAD), bf),
                pltpu.VMEM((HEADS, t, HEAD), bf), pltpu.VMEM((t, d), f32),
                dma((2 * KV + HEADS,)), dma((d // HEAD,)), dma((2 * KV,)), dma((2 * KV,)), dma((HEADS,)), dma((8,)), dma((8,)), dma((8,)),
                dma((DEVICES,)), dma((DEVICES,)), dma((8,)), dma((HEADS,)),
            ],
            compiler_params=pltpu.CompilerParams(has_side_effects=True, vmem_limit_bytes=VMEM),
            name="attention",
        )(x, gain[None], *turns, wk, wv, wq, wo)

    tokens, whole = P(("dp", "sp"), None), P(None, None)
    return jax.shard_map(
        step,
        mesh=mesh,
        in_specs=(tokens, P(None), whole, whole, whole, whole),
        out_specs=tokens,
        check_vma=False,
    )
```

```python
import functools

import jax
import jax.numpy as jnp
import numpy as np
from jax import lax
from jax.experimental import pallas as pl
from jax.experimental.pallas import tpu as pltpu
from jax.sharding import PartitionSpec as P

NEG = -1e30
HIDDEN = 2 * NEG
LOG2E = 1.4426950408889634
HEAD = 256
THETA = 10000
KV = 4
HEADS = 8
DEVICES = 16
VMEM = 63 * 2**20


def _dot(a, b, ca, cb):
    return lax.dot_general(a, b, (((ca,), (cb,)), ((), ())), preferred_element_type=jnp.float32)


def _kernel(x_ref, gain_ref, turn_ref, start_ref, wk, wv, wq, wo, y_ref, a_s, cos_s, sin_s, wk_s, wv_s, wq_s, k_own, v_own, q_own, k_r, v_r,
            q_r, acc, top_s, o_s, o_r, y_s, w_sem, wo_sem, k_send, v_send, q_send, o_send, kf_send, vf_send, k_recv, v_recv, q_recv, o_recv):
    t, d = x_ref.shape
    width = HEADS * HEAD
    rows = min(t, 256)
    me, dp = lax.axis_index("sp"), lax.axis_index("dp")
    core = lax.rem(me, 2)
    z = lax.rem(lax.div(me, 2), 4)
    y = lax.div(me, 8)
    side = lax.div(z, 2)
    slot = y * 4 + lax.rem(z, 2) * 2 + core
    head = y * 2 + lax.rem(z, 2)
    inner = (z == 1) | (z == 2)

    def columns_of(n):
        return pl.ds(pl.multiple_of(n * HEAD, HEAD), HEAD)

    def weights(n):
        yield wk.at[:, columns_of(n)], wk_s.at[n], w_sem.at[n]
        yield wv.at[:, columns_of(n)], wv_s.at[n], w_sem.at[KV + n]
        for i in range(2):
            at = pl.ds(pl.multiple_of((2 * n + i) * d, 256), d)
            yield wq.at[:, columns_of(2 * n + i)], wq_s.at[at, :], w_sem.at[2 * KV + 2 * n + i]

    def nth(n):
        return lax.rem(n + 2 * y, KV)

    def arrived(ref, sem):
        pltpu.make_async_copy(ref, ref, sem).wait()

    barrier = pltpu.get_barrier_semaphore()
    for i in range(1, DEVICES):
        pl.semaphore_signal(barrier, inc=1, device_id=(dp, lax.rem(me + i, DEVICES)), device_id_type=pl.DeviceIdType.MESH)
    for n in range(KV):
        for copy in weights(nth(n)):
            pltpu.make_async_copy(*copy).start()

    def norm(r, _):
        at = pl.ds(r * rows, rows)
        wide = x_ref[at, :].astype(jnp.float32)
        scale = lax.rsqrt(jnp.mean(wide * wide, -1, keepdims=True) + 1e-6)
        a_s[at, :] = (wide * scale * gain_ref[...].astype(jnp.float32)).astype(jnp.bfloat16)

    lax.fori_loop(0, t // rows, norm, None)

    cos_a, sin_a = start_ref[me][:1, : HEAD // 2], start_ref[me][:1, HEAD // 2 :]
    cos_b, sin_b = turn_ref[:, : HEAD // 2], turn_ref[:, HEAD // 2 :]
    cos_s[...] = cos_a * cos_b - sin_a * sin_b
    sin_s[...] = sin_a * cos_b + cos_a * sin_b

    def turned(r, at):
        half = HEAD // 2
        cos, sin = cos_s[at, :], sin_s[at, :]
        a, b = r[:, :half].astype(jnp.float32), r[:, half:].astype(jnp.float32)
        return jnp.concatenate([a * cos - b * sin, b * cos + a * sin], -1).astype(jnp.bfloat16)

    def project(w):
        for r in range(t // rows):
            at = pl.ds(r * rows, rows)
            yield at, _dot(a_s[at, :], w, 1, 0).astype(jnp.bfloat16)

    def deliver(src, dst, send, recv, to):
        @pl.when(to == me)
        def _():
            pltpu.make_async_copy(src, dst, recv).start()

        @pl.when(to != me)
        def _():
            pltpu.make_async_remote_copy(src_ref=src, dst_ref=dst, send_sem=send, recv_sem=recv, device_id=(dp, to),
                                         device_id_type=pl.DeviceIdType.MESH).start()

    def kv_to(n, s):
        return lax.div(n, 2) * 8 + s * 4 + lax.rem(n, 2) * 2 + core

    def q_to(n):
        return lax.div(n, 4) * 8 + side * 4 + lax.rem(lax.div(n, 2), 2) * 2 + lax.rem(n, 2)


    def send_kv(n, s):
        deliver(k_own.at[n], k_r.at[me], k_send.at[n * 2 + s], k_recv.at[me], kv_to(n, s))
        deliver(v_own.at[n], v_r.at[me], v_send.at[n * 2 + s], v_recv.at[me], kv_to(n, s))

    def over(n):
        @pl.when((side == 0) | (me < 12))
        def _():
            send_kv(n, 1 - side)

    def make_q(n, _):
        arrived(wk_s.at[0], w_sem.at[2 * KV + n])
        for at, r in project(wq_s[pl.ds(pl.multiple_of(n * d, 256), d), :]):
            q_own[n, at, :] = turned(r, at)
        deliver(q_own.at[n], q_r.at[slot], q_send.at[n], q_recv.at[slot], q_to(n))

    def make(i, _):
        n = nth(i)
        arrived(wk_s.at[n], w_sem.at[n])
        for at, r in project(wk_s[n]):
            k_own[n, at, :] = turned(r, at)
        arrived(wv_s.at[n], w_sem.at[KV + n])
        for at, r in project(wv_s[n]):
            v_own[n, :, at] = r.T

        @pl.when(inner)
        def _():
            over(n)

        lax.fori_loop(2 * n, 2 * n + 2, make_q, None)

    pl.semaphore_wait(barrier, DEVICES - 1)
    lax.fori_loop(0, KV, make, None)
    lax.fori_loop(0, KV, lambda n, _: send_kv(nth(n), side), None)

    def out_weights(n):
        at = pl.ds(n * HEAD, HEAD) if isinstance(n, int) else pl.ds(pl.multiple_of(n * HEAD, HEAD), HEAD)
        to = pl.ds(pl.multiple_of(n * width, width), width)
        return pltpu.make_async_copy(wo.at[:, at], wq_s.at[to, :], wo_sem.at[n])

    lax.fori_loop(0, d // HEAD, lambda n, _: out_weights(n).start(), None)

    @pl.when(jnp.logical_not(inner))
    def _():
        lax.fori_loop(0, KV, lambda n, _: over(nth(n)), None)

    for i in range(8):
        top_s[i] = jnp.full((1, t), NEG, jnp.float32)
        acc[i] = jnp.zeros((HEAD + 8, t), jnp.float32)
    lax.fori_loop(0, 8, lambda i, _: arrived(q_r.at[i], q_recv.at[i]), None)

    e = HEAD**-0.5 * LOG2E
    ones = jnp.ones((8, t), jnp.bfloat16)

    def block(kb, g, masked):
        at = [g * 4 + n for n in range(4)]
        scores = [_dot(k_r[kb], q_r[i], 1, 1) for i in at]
        if masked:
            gap = lax.broadcasted_iota(jnp.int32, (t, t), 1) - lax.broadcasted_iota(jnp.int32, (t, t), 0)
            first = (g * 8 + side * 4 - kb) * t
            scores = [jnp.where(gap >= -(first + n * t), s, HIDDEN) for n, s in enumerate(scores)]
        weights, keeps = [], []
        for i, s in zip(at, scores):
            old = top_s[i]
            top = jnp.maximum(old, s.max(axis=0, keepdims=True))
            top_s[i] = top
            weights.append(jnp.exp2((s - top) * e).astype(jnp.bfloat16))
            keeps.append(jnp.exp2((old - top) * e))
        values = jnp.concatenate([v_r[kb], ones], axis=0)
        for i, p, keep in zip(at, weights, keeps):
            acc[i] = acc[i] * keep + _dot(values, p, 1, 0)

    def attend(kb):
        def row(g, _):
            first = g * 8 + side * 4

            @pl.when(kb < first)
            def _():
                block(kb, g, False)

            @pl.when((kb >= first) & (kb < first + 4))
            def _():
                block(kb, g, True)

        lax.fori_loop(0, 2, row, None)

    def finish(n, _):
        m = lax.rem(n, 4)
        i = n - m + lax.rem(m + 2 - 2 * lax.rem(z, 2), 4)
        o_s[i] = (acc[i, :HEAD, :] * (1 / acc[i, HEAD : HEAD + 1, :])).T.astype(jnp.bfloat16)
        to = lax.div(i, 4) * 8 + side * 4 + lax.rem(i, 4)
        j = head * 2 + core
        deliver(o_s.at[i], o_r.at[j], o_send.at[i], o_recv.at[j], to)

    def chip_at(m):
        pair, second = lax.div(m, 2), lax.rem(m, 2)
        across = 4 * side + 1 - z
        near, far = 2 - side, 3 - 3 * side
        second_column, third_column = jnp.where(side == 1, near, across), jnp.where(side == 1, across, near)
        column = jnp.where(pair == 0, z, jnp.where(pair == 1, second_column, jnp.where(pair == 2, third_column, far)))
        row = jnp.where(pair == 3, second, jnp.where(second == 0, y, 1 - y))
        return row * 8 + column * 2

    def chip(m, _):
        base = chip_at(m)

        @pl.when((side == 1) | (base < 12))
        def _():
            mine, other = base + core, base + 1 - core
            arrived(k_r.at[mine], k_recv.at[mine])
            arrived(v_r.at[mine], v_recv.at[mine])
            sibling = me + 1 - 2 * core
            for ref, send, recv in ((k_r, kf_send, k_recv), (v_r, vf_send, v_recv)):
                pltpu.make_async_remote_copy(src_ref=ref.at[mine], dst_ref=ref.at[mine], send_sem=send.at[m], recv_sem=recv.at[mine],
                                             device_id=(dp, sibling), device_id_type=pl.DeviceIdType.MESH).start()
            attend(mine)
            arrived(k_r.at[other], k_recv.at[other])
            arrived(v_r.at[other], v_recv.at[other])
            attend(other)

        done = m == jnp.where(side == 0, 3, 6)

        @pl.when(done | (m == 7))
        def _():
            at = jnp.where(done, 0, 4)
            lax.fori_loop(at, at + 4, finish, None)

    lax.fori_loop(0, 8, chip, None)

    for i in range(4):
        j = (lax.rem(y + i % 2, 2) * 2 + lax.rem(lax.rem(z, 2) + i // 2, 2)) * 2
        for n in range(2):
            arrived(o_s.at[0], o_recv.at[j + n])

        def columns(n, _):
            at = pl.ds(pl.multiple_of(n * HEAD, HEAD), HEAD)
            if i == 0:
                out_weights(n).wait()
            w = wq_s[pl.ds(pl.multiple_of(n * width + j * HEAD, 2 * HEAD), 2 * HEAD), :]
            part = _dot(o_r[j], w[:HEAD], 1, 0) + _dot(o_r[j + 1], w[HEAD:], 1, 0)
            part += x_ref[:, at].astype(jnp.float32) if i == 0 else y_s[:, at]
            if i < 3:
                y_s[:, at] = part
            else:
                y_ref[:, at] = part.astype(jnp.bfloat16)

        lax.fori_loop(0, d // HEAD, columns, None)

    def left(ref, sem):
        pltpu.make_async_copy(ref, ref, sem).wait()

    def ends(n, _):
        for s in range(2):
            @pl.when((kv_to(n, s) != me) & ((s == side) | (side == 0) | (me < 12)))
            def _():
                left(k_own.at[n], k_send.at[n * 2 + s])
                left(v_own.at[n], v_send.at[n * 2 + s])

    lax.fori_loop(0, KV, ends, None)

    def q_ends(n, _):
        @pl.when(q_to(n) != me)
        def _():
            left(q_own.at[n], q_send.at[n])

        @pl.when(n != slot)
        def _():
            left(o_s.at[n], o_send.at[n])


    lax.fori_loop(0, HEADS, q_ends, None)

    def f_ends(m, _):
        base = chip_at(m)

        @pl.when((side == 1) | (base < 12))
        def _():
            left(k_r.at[0], kf_send.at[m])
            left(v_r.at[0], vf_send.at[m])

    lax.fori_loop(0, 8, f_ends, None)


def solution(mesh):
    def step(x, gain, wq, wk, wv, wo):
        t, d = x.shape
        half = HEAD // 2
        power = float(THETA) ** (-np.arange(half) / half)
        turns = [np.concatenate([np.cos(a), np.sin(a)], 1).astype(np.float32) for a in (np.arange(t)[:, None] * power,
                                                                                      np.arange(DEVICES)[:, None] * t * power)]
        turns[1] = np.repeat(turns[1][:, None], 8, 1)
        bf, f32, dma = jnp.bfloat16, jnp.float32, pltpu.SemaphoreType.DMA
        vmem, hbm = pl.BlockSpec(memory_space=pltpu.VMEM), pl.BlockSpec(memory_space=pl.ANY)
        return pl.pallas_call(
            _kernel,
            in_specs=[vmem] * 4 + [hbm] * 4,
            out_specs=vmem,
            out_shape=jax.ShapeDtypeStruct((t, d), bf),
            scratch_shapes=[
                pltpu.VMEM((t, d), bf), pltpu.VMEM((t, half), f32), pltpu.VMEM((t, half), f32),
                pltpu.VMEM((KV, d, HEAD), bf), pltpu.VMEM((KV, d, HEAD), bf), pltpu.VMEM((HEADS * d, HEAD), bf),
                pltpu.VMEM((KV, t, HEAD), bf), pltpu.VMEM((KV, HEAD, t), bf), pltpu.VMEM((HEADS, t, HEAD), bf),
                pltpu.VMEM((DEVICES, t, HEAD), bf), pltpu.VMEM((DEVICES, HEAD, t), bf), pltpu.VMEM((8, t, HEAD), bf),
                pltpu.VMEM((8, HEAD + 8, t), f32), pltpu.VMEM((8, 1, t), f32), pltpu.VMEM((8, t, HEAD), bf),
                pltpu.VMEM((HEADS, t, HEAD), bf), pltpu.VMEM((t, d), f32),
                dma((2 * KV + HEADS,)), dma((d // HEAD,)), dma((2 * KV,)), dma((2 * KV,)), dma((HEADS,)), dma((8,)), dma((8,)), dma((8,)),
                dma((DEVICES,)), dma((DEVICES,)), dma((8,)), dma((HEADS,)),
            ],
            compiler_params=pltpu.CompilerParams(has_side_effects=True, collective_id=0, vmem_limit_bytes=VMEM),
            name="attention",
        )(x, gain[None], *turns, wk, wv, wq, wo)

    tokens, whole = P(("dp", "sp"), None), P(None, None)
    return jax.shard_map(
        step,
        mesh=mesh,
        in_specs=(tokens, P(None), whole, whole, whole, whole),
        out_specs=tokens,
        check_vma=False,
    )
```

```python
import functools

import jax
import jax.numpy as jnp
import numpy as np
from jax import lax
from jax.experimental import pallas as pl
from jax.experimental.pallas import tpu as pltpu
from jax.sharding import PartitionSpec as P

NEG = -1e30
HIDDEN = 2 * NEG
LOG2E = 1.4426950408889634
HEAD = 256
THETA = 10000
KV = 4
HEADS = 8
DEVICES = 16
VMEM = 63 * 2**20


def _dot(a, b, ca, cb):
    return lax.dot_general(a, b, (((ca,), (cb,)), ((), ())), preferred_element_type=jnp.float32)


def _kernel(x_ref, gain_ref, turn_ref, start_ref, wk, wv, wq, wo, y_ref, a_s, cos_s, sin_s, wk_s, wv_s, wq_s, k_own, v_own, q_own, k_r, v_r,
            q_r, acc, top_s, o_s, o_r, y_s, w_sem, wo_sem, k_send, v_send, q_send, o_send, kf_send, vf_send, k_recv, v_recv, q_recv, o_recv):
    t, d = x_ref.shape
    width = HEADS * HEAD
    rows = min(t, 256)
    me, dp = lax.axis_index("sp"), lax.axis_index("dp")
    core = lax.rem(me, 2)
    z = lax.rem(lax.div(me, 2), 4)
    y = lax.div(me, 8)
    side = lax.div(z, 2)
    slot = y * 4 + lax.rem(z, 2) * 2 + core
    head = y * 2 + lax.rem(z, 2)
    inner = (z == 1) | (z == 2)

    def columns_of(n):
        return pl.ds(pl.multiple_of(n * HEAD, HEAD), HEAD)

    def weights(n):
        yield wk.at[:, columns_of(n)], wk_s.at[n], w_sem.at[n]
        yield wv.at[:, columns_of(n)], wv_s.at[n], w_sem.at[KV + n]
        for i in range(2):
            at = pl.ds(pl.multiple_of((2 * n + i) * d, 256), d)
            yield wq.at[:, columns_of(2 * n + i)], wq_s.at[at, :], w_sem.at[2 * KV + 2 * n + i]

    def nth(n):
        return lax.rem(n + 2 * y, KV)

    def arrived(ref, sem):
        pltpu.make_async_copy(ref, ref, sem).wait()

    barrier = pltpu.get_barrier_semaphore()
    for i in range(1, DEVICES):
        pl.semaphore_signal(barrier, inc=1, device_id=(dp, lax.rem(me + i, DEVICES)), device_id_type=pl.DeviceIdType.MESH)
    def fetch(n, kinds):
        for kind, copy in enumerate(weights(n)):
            if kind in kinds:
                pltpu.make_async_copy(*copy).start()

    fetch(nth(0), (0, 1))
    for n in range(KV):
        fetch(nth(n + 2), (2, 3))
    for n in range(1, KV):
        fetch(nth(n), (0, 1))

    def norm(r, _):
        at = pl.ds(r * rows, rows)
        wide = x_ref[at, :].astype(jnp.float32)
        scale = lax.rsqrt(jnp.mean(wide * wide, -1, keepdims=True) + 1e-6)
        a_s[at, :] = (wide * scale * gain_ref[...].astype(jnp.float32)[None]).astype(jnp.bfloat16)

    lax.fori_loop(0, t // rows, norm, None)

    cos_a, sin_a = start_ref[me][:1, : HEAD // 2], start_ref[me][:1, HEAD // 2 :]
    cos_b, sin_b = turn_ref[:, : HEAD // 2], turn_ref[:, HEAD // 2 :]
    cos_s[...] = cos_a * cos_b - sin_a * sin_b
    sin_s[...] = sin_a * cos_b + cos_a * sin_b

    def turned(r, at):
        half = HEAD // 2
        cos, sin = cos_s[at, :], sin_s[at, :]
        a, b = r[:, :half].astype(jnp.float32), r[:, half:].astype(jnp.float32)
        return jnp.concatenate([a * cos - b * sin, b * cos + a * sin], -1).astype(jnp.bfloat16)

    def project(w):
        for r in range(t // rows):
            at = pl.ds(r * rows, rows)
            yield at, _dot(a_s[at, :], w, 1, 0).astype(jnp.bfloat16)

    def deliver(src, dst, send, recv, to):
        @pl.when(to == me)
        def _():
            pltpu.make_async_copy(src, dst, recv).start()

        @pl.when(to != me)
        def _():
            pltpu.make_async_remote_copy(src_ref=src, dst_ref=dst, send_sem=send, recv_sem=recv, device_id=(dp, to),
                                         device_id_type=pl.DeviceIdType.MESH).start()

    def kv_to(n, s):
        return lax.div(n, 2) * 8 + s * 4 + lax.rem(n, 2) * 2 + core

    def q_to(n):
        return lax.div(n, 4) * 8 + side * 4 + lax.rem(lax.div(n, 2), 2) * 2 + lax.rem(n, 2)


    def send_kv(n, s):
        deliver(k_own.at[n], k_r.at[me], k_send.at[n * 2 + s], k_recv.at[me], kv_to(n, s))
        deliver(v_own.at[n], v_r.at[me], v_send.at[n * 2 + s], v_recv.at[me], kv_to(n, s))

    def over(n):
        @pl.when((side == 0) | (me < 12))
        def _():
            send_kv(n, 1 - side)

    def make_q(i, _):
        n = lax.rem(i + 4 * (1 - y), HEADS)
        arrived(wk_s.at[0], w_sem.at[2 * KV + n])
        for at, r in project(wq_s[pl.ds(pl.multiple_of(n * d, 256), d), :]):
            q_own[n, at, :] = turned(r, at)
        deliver(q_own.at[n], q_r.at[slot], q_send.at[n], q_recv.at[slot], q_to(n))

    def make(i, _):
        n = nth(i)
        arrived(wk_s.at[n], w_sem.at[n])
        for at, r in project(wk_s[n]):
            k_own[n, at, :] = turned(r, at)
        arrived(wv_s.at[n], w_sem.at[KV + n])
        for at, r in project(wv_s[n]):
            v_own[n, :, at] = r.T

        @pl.when(inner)
        def _():
            over(n)

    pl.semaphore_wait(barrier, DEVICES - 1)
    lax.fori_loop(0, 1, make, None)
    lax.fori_loop(0, HEADS, make_q, None)
    lax.fori_loop(1, KV, make, None)
    lax.fori_loop(0, KV, lambda n, _: send_kv(nth(n), side), None)

    def out_weights(n):
        at = pl.ds(n * HEAD, HEAD) if isinstance(n, int) else pl.ds(pl.multiple_of(n * HEAD, HEAD), HEAD)
        to = pl.ds(pl.multiple_of(n * width, width), width)
        return pltpu.make_async_copy(wo.at[:, at], wq_s.at[to, :], wo_sem.at[n])

    lax.fori_loop(0, d // HEAD, lambda n, _: out_weights(n).start(), None)

    @pl.when(jnp.logical_not(inner))
    def _():
        lax.fori_loop(0, KV, lambda n, _: over(nth(n)), None)

    for i in range(8):
        top_s[i] = jnp.full((1, t), NEG, jnp.float32)
        acc[i] = jnp.zeros((HEAD + 8, t), jnp.float32)
    lax.fori_loop(0, 8, lambda i, _: arrived(q_r.at[i], q_recv.at[i]), None)

    e = HEAD**-0.5 * LOG2E
    ones = jnp.ones((8, t), jnp.bfloat16)

    def block(kb, g, masked):
        at = [g * 4 + n for n in range(4)]
        scores = [_dot(k_r[kb], q_r[i], 1, 1) for i in at]
        if masked:
            gap = lax.broadcasted_iota(jnp.int32, (t, t), 1) - lax.broadcasted_iota(jnp.int32, (t, t), 0)
            first = (g * 8 + side * 4 - kb) * t
            scores = [jnp.where(gap >= -(first + n * t), s, HIDDEN) for n, s in enumerate(scores)]
        weights, keeps = [], []
        for i, s in zip(at, scores):
            old = top_s[i]
            top = jnp.maximum(old, s.max(axis=0, keepdims=True))
            top_s[i] = top
            weights.append(jnp.exp2((s - top) * e).astype(jnp.bfloat16))
            keeps.append(jnp.exp2((old - top) * e))
        values = jnp.concatenate([v_r[kb], ones], axis=0)
        for i, p, keep in zip(at, weights, keeps):
            acc[i] = acc[i] * keep + _dot(values, p, 1, 0)

    def attend(kb, g):
        first = g * 8 + side * 4

        @pl.when(kb < first)
        def _():
            block(kb, g, False)

        @pl.when((kb >= first) & (kb < first + 4))
        def _():
            block(kb, g, True)

    def finish(n, _):
        m = lax.rem(n, 4)
        i = n - m + lax.rem(m + 2 - 2 * lax.rem(z, 2), 4)
        o_s[i] = (acc[i, :HEAD, :] * (1 / acc[i, HEAD : HEAD + 1, :])).T.astype(jnp.bfloat16)
        to = lax.div(i, 4) * 8 + side * 4 + lax.rem(i, 4)
        j = head * 2 + core
        deliver(o_s.at[i], o_r.at[j], o_send.at[i], o_recv.at[j], to)

    def row_of(m):
        return jnp.where(lax.rem(m, 2) == 0, y, 1 - y)

    def chip_at(m):
        pair = lax.div(m, 2)
        across = 4 * side + 1 - z
        near, far = 2 - side, 3 - 3 * side
        second_column, third_column = jnp.where(side == 1, near, across), jnp.where(side == 1, across, near)
        column = jnp.where(pair == 0, z, jnp.where(pair == 1, second_column, jnp.where(pair == 2, third_column, far)))
        return row_of(m) * 8 + column * 2

    def chip(m, _):
        base = chip_at(m)

        @pl.when((side == 1) | (base < 12))
        def _():
            mine, other = base + core, base + 1 - core
            arrived(k_r.at[mine], k_recv.at[mine])
            arrived(v_r.at[mine], v_recv.at[mine])
            sibling = me + 1 - 2 * core
            for ref, send, recv in ((k_r, kf_send, k_recv), (v_r, vf_send, v_recv)):
                pltpu.make_async_remote_copy(src_ref=ref.at[mine], dst_ref=ref.at[mine], send_sem=send.at[m], recv_sem=recv.at[mine],
                                             device_id=(dp, sibling), device_id_type=pl.DeviceIdType.MESH).start()
            last = (side == 1) & (m == 7)

            def part(i, _):
                half = jnp.where(last, lax.rem(i, 2), lax.div(i, 2))
                g = jnp.where(last, lax.div(i, 2), lax.rem(i, 2))

                @pl.when(i == jnp.where(last, 1, 2))
                def _():
                    arrived(k_r.at[other], k_recv.at[other])
                    arrived(v_r.at[other], v_recv.at[other])

                attend(jnp.where(half == 0, mine, other), g)

                @pl.when(last & (i == 1) & (row_of(m) == 0))
                def _():
                    lax.fori_loop(0, 4, finish, None)

            lax.fori_loop(0, 4, part, None)

        @pl.when(m == jnp.where(side == 0, 3, jnp.where(y == 0, 6, 8)))
        def _():
            lax.fori_loop(0, 4, finish, None)

        @pl.when(m == 7)
        def _():
            lax.fori_loop(4, 8, finish, None)

    lax.fori_loop(0, 8, chip, None)

    for i in range(4):
        j = (lax.rem(y + i % 2, 2) * 2 + lax.rem(lax.rem(z, 2) + i // 2, 2)) * 2
        for n in range(2):
            arrived(o_s.at[0], o_recv.at[j + n])

        def columns(n, _):
            at = pl.ds(pl.multiple_of(n * HEAD, HEAD), HEAD)
            if i == 0:
                out_weights(n).wait()
            w = wq_s[pl.ds(pl.multiple_of(n * width + j * HEAD, 2 * HEAD), 2 * HEAD), :]
            part = _dot(o_r[j], w[:HEAD], 1, 0) + _dot(o_r[j + 1], w[HEAD:], 1, 0)
            part += x_ref[:, at].astype(jnp.float32) if i == 0 else y_s[:, at]
            if i < 3:
                y_s[:, at] = part
            else:
                y_ref[:, at] = part.astype(jnp.bfloat16)

        lax.fori_loop(0, d // HEAD, columns, None)

    def left(ref, sem):
        pltpu.make_async_copy(ref, ref, sem).wait()

    def ends(n, _):
        for s in range(2):
            @pl.when((kv_to(n, s) != me) & ((s == side) | (side == 0) | (me < 12)))
            def _():
                left(k_own.at[n], k_send.at[n * 2 + s])
                left(v_own.at[n], v_send.at[n * 2 + s])

    lax.fori_loop(0, KV, ends, None)

    def q_ends(n, _):
        @pl.when(q_to(n) != me)
        def _():
            left(q_own.at[n], q_send.at[n])

        @pl.when(n != slot)
        def _():
            left(o_s.at[n], o_send.at[n])


    lax.fori_loop(0, HEADS, q_ends, None)

    def f_ends(m, _):
        base = chip_at(m)

        @pl.when((side == 1) | (base < 12))
        def _():
            left(k_r.at[0], kf_send.at[m])
            left(v_r.at[0], vf_send.at[m])

    lax.fori_loop(0, 8, f_ends, None)


def solution(mesh):
    def step(x, gain, wq, wk, wv, wo):
        t, d = x.shape
        half = HEAD // 2
        power = float(THETA) ** (-np.arange(half) / half)
        turns = [np.concatenate([np.cos(a), np.sin(a)], 1).astype(np.float32) for a in (np.arange(t)[:, None] * power,
                                                                                      np.arange(DEVICES)[:, None] * t * power)]
        turns[1] = np.repeat(turns[1][:, None], 8, 1)
        bf, f32, dma = jnp.bfloat16, jnp.float32, pltpu.SemaphoreType.DMA
        vmem, hbm = pl.BlockSpec(memory_space=pltpu.VMEM), pl.BlockSpec(memory_space=pl.ANY)
        return pl.pallas_call(
            _kernel,
            in_specs=[vmem] * 4 + [hbm] * 4,
            out_specs=vmem,
            out_shape=jax.ShapeDtypeStruct((t, d), bf),
            scratch_shapes=[
                pltpu.VMEM((t, d), bf), pltpu.VMEM((t, half), f32), pltpu.VMEM((t, half), f32),
                pltpu.VMEM((KV, d, HEAD), bf), pltpu.VMEM((KV, d, HEAD), bf), pltpu.VMEM((HEADS * d, HEAD), bf),
                pltpu.VMEM((KV, t, HEAD), bf), pltpu.VMEM((KV, HEAD, t), bf), pltpu.VMEM((HEADS, t, HEAD), bf),
                pltpu.VMEM((DEVICES, t, HEAD), bf), pltpu.VMEM((DEVICES, HEAD, t), bf), pltpu.VMEM((8, t, HEAD), bf),
                pltpu.VMEM((8, HEAD + 8, t), f32), pltpu.VMEM((8, 1, t), f32), pltpu.VMEM((8, t, HEAD), bf),
                pltpu.VMEM((HEADS, t, HEAD), bf), pltpu.VMEM((t, d), f32),
                dma((2 * KV + HEADS,)), dma((d // HEAD,)), dma((2 * KV,)), dma((2 * KV,)), dma((HEADS,)), dma((8,)), dma((8,)), dma((8,)),
                dma((DEVICES,)), dma((DEVICES,)), dma((8,)), dma((HEADS,)),
            ],
            compiler_params=pltpu.CompilerParams(has_side_effects=True, collective_id=0, vmem_limit_bytes=VMEM),
            name="attention",
        )(x, gain, *turns, wk, wv, wq, wo)

    tokens, whole = P(("dp", "sp"), None), P(None, None)
    return jax.shard_map(
        step,
        mesh=mesh,
        in_specs=(tokens, P(None), whole, whole, whole, whole),
        out_specs=tokens,
        check_vma=False,
    )
```

```python
import functools

import jax
import jax.numpy as jnp
import numpy as np
from jax import lax
from jax.experimental import pallas as pl
from jax.experimental.pallas import tpu as pltpu
from jax.sharding import PartitionSpec as P

NEG = -1e30
HIDDEN = 2 * NEG
LOG2E = 1.4426950408889634
HEAD = 256
THETA = 10000
KV = 4
HEADS = 8
DEVICES = 16
VMEM = 63 * 2**20


def _dot(a, b, ca, cb):
    return lax.dot_general(a, b, (((ca,), (cb,)), ((), ())), preferred_element_type=jnp.float32)


def _kernel(x_ref, gain_ref, turn_ref, start_ref, wk, wv, wq, wo, y_ref, a_s, cos_s, sin_s, wk_s, wv_s, wq_s, k_own, v_own, q_own, k_r, v_r,
            q_r, acc, top_s, o_s, o_r, y_s, w_sem, wo_sem, k_send, v_send, q_send, o_send, kf_send, vf_send, k_recv, v_recv, q_recv, o_recv):
    t, d = x_ref.shape
    width = HEADS * HEAD
    rows = min(t, 256)
    me, dp = lax.axis_index("sp"), lax.axis_index("dp")
    core = lax.rem(me, 2)
    z = lax.rem(lax.div(me, 2), 4)
    y = lax.div(me, 8)
    side = lax.div(z, 2)
    slot = y * 4 + lax.rem(z, 2) * 2 + core
    head = y * 2 + lax.rem(z, 2)
    inner = (z == 1) | (z == 2)

    def columns_of(n):
        return pl.ds(pl.multiple_of(n * HEAD, HEAD), HEAD)

    def weights(n):
        yield wk.at[:, columns_of(n)], wk_s.at[n], w_sem.at[n]
        yield wv.at[:, columns_of(n)], wv_s.at[n], w_sem.at[KV + n]
        for i in range(2):
            at = pl.ds(pl.multiple_of((2 * n + i) * d, 256), d)
            yield wq.at[:, columns_of(2 * n + i)], wq_s.at[at, :], w_sem.at[2 * KV + 2 * n + i]

    def nth(n):
        return lax.rem(n + 2 * y, KV)

    def arrived(ref, sem):
        pltpu.make_async_copy(ref, ref, sem).wait()

    barrier = pltpu.get_barrier_semaphore()
    for i in range(1, DEVICES):
        pl.semaphore_signal(barrier, inc=1, device_id=(dp, lax.rem(me + i, DEVICES)), device_id_type=pl.DeviceIdType.MESH)
    def fetch(n, kinds):
        for kind, copy in enumerate(weights(n)):
            if kind in kinds:
                pltpu.make_async_copy(*copy).start()

    fetch(nth(0), (0, 1))
    for n in range(KV):
        fetch(nth(n + 2), (2, 3))
    for n in range(1, KV):
        fetch(nth(n), (0, 1))

    def norm(r, _):
        at = pl.ds(r * rows, rows)
        wide = x_ref[at, :].astype(jnp.float32)
        scale = lax.rsqrt(jnp.mean(wide * wide, -1, keepdims=True) + 1e-6)
        a_s[at, :] = (wide * scale * gain_ref[...].astype(jnp.float32)[None]).astype(jnp.bfloat16)

    lax.fori_loop(0, t // rows, norm, None)

    cos_a, sin_a = start_ref[me][:1, : HEAD // 2], start_ref[me][:1, HEAD // 2 :]
    cos_b, sin_b = turn_ref[:, : HEAD // 2], turn_ref[:, HEAD // 2 :]
    cos_s[...] = cos_a * cos_b - sin_a * sin_b
    sin_s[...] = sin_a * cos_b + cos_a * sin_b

    def turned(r, at):
        half = HEAD // 2
        cos, sin = cos_s[at, :], sin_s[at, :]
        a, b = r[:, :half].astype(jnp.float32), r[:, half:].astype(jnp.float32)
        return jnp.concatenate([a * cos - b * sin, b * cos + a * sin], -1).astype(jnp.bfloat16)

    def project(w):
        for r in range(t // rows):
            at = pl.ds(r * rows, rows)
            yield at, _dot(a_s[at, :], w, 1, 0).astype(jnp.bfloat16)

    def deliver(src, dst, send, recv, to):
        @pl.when(to == me)
        def _():
            pltpu.make_async_copy(src, dst, recv).start()

        @pl.when(to != me)
        def _():
            pltpu.make_async_remote_copy(src_ref=src, dst_ref=dst, send_sem=send, recv_sem=recv, device_id=(dp, to),
                                         device_id_type=pl.DeviceIdType.MESH).start()

    def kv_to(n, s):
        return lax.div(n, 2) * 8 + s * 4 + lax.rem(n, 2) * 2 + core

    def q_to(n):
        return lax.div(n, 4) * 8 + side * 4 + lax.rem(lax.div(n, 2), 2) * 2 + lax.rem(n, 2)


    def send_kv(n, s):
        deliver(k_own.at[n], k_r.at[me], k_send.at[n * 2 + s], k_recv.at[me], kv_to(n, s))
        deliver(v_own.at[n], v_r.at[me], v_send.at[n * 2 + s], v_recv.at[me], kv_to(n, s))

    def over(n):
        @pl.when((side == 0) | (me < 12))
        def _():
            send_kv(n, 1 - side)

    def make_q(i, _):
        n = lax.rem(i + 4 * (1 - y), HEADS)
        arrived(wk_s.at[0], w_sem.at[2 * KV + n])
        for at, r in project(wq_s[pl.ds(pl.multiple_of(n * d, 256), d), :]):
            q_own[n, at, :] = turned(r, at)
        deliver(q_own.at[n], q_r.at[slot], q_send.at[n], q_recv.at[slot], q_to(n))

    def make(i, _):
        n = nth(i)
        arrived(wk_s.at[n], w_sem.at[n])
        for at, r in project(wk_s[n]):
            k_own[n, at, :] = turned(r, at)
        arrived(wv_s.at[n], w_sem.at[KV + n])
        for at, r in project(wv_s[n]):
            v_own[n, :, at] = r.T

        @pl.when(inner)
        def _():
            over(n)

    pl.semaphore_wait(barrier, DEVICES - 1)
    lax.fori_loop(0, 1, make, None)
    lax.fori_loop(0, HEADS, make_q, None)
    lax.fori_loop(1, KV, make, None)
    lax.fori_loop(0, KV, lambda n, _: send_kv(nth(n), side), None)

    def out_weights(n):
        at = pl.ds(n * HEAD, HEAD) if isinstance(n, int) else pl.ds(pl.multiple_of(n * HEAD, HEAD), HEAD)
        to = pl.ds(pl.multiple_of(n * width, width), width)
        return pltpu.make_async_copy(wo.at[:, at], wq_s.at[to, :], wo_sem.at[n])

    lax.fori_loop(0, d // HEAD, lambda n, _: out_weights(n).start(), None)

    @pl.when(jnp.logical_not(inner))
    def _():
        lax.fori_loop(0, KV, lambda n, _: over(nth(n)), None)

    for i in range(8):
        top_s[i] = jnp.full((1, t), NEG, jnp.float32)
        acc[i] = jnp.zeros((HEAD + 8, t), jnp.float32)
    lax.fori_loop(0, 8, lambda i, _: arrived(q_r.at[i], q_recv.at[i]), None)

    e = HEAD**-0.5 * LOG2E
    ones = jnp.ones((8, t), jnp.bfloat16)

    def block(kb, g, masked):
        at = [g * 4 + n for n in range(4)]
        scores = [_dot(k_r[kb], q_r[i], 1, 1) for i in at]
        if masked:
            gap = lax.broadcasted_iota(jnp.int32, (t, t), 1) - lax.broadcasted_iota(jnp.int32, (t, t), 0)
            first = (g * 8 + side * 4 - kb) * t
            scores = [jnp.where(gap >= -(first + n * t), s, HIDDEN) for n, s in enumerate(scores)]
        weights, keeps = [], []
        for i, s in zip(at, scores):
            old = top_s[i]
            top = jnp.maximum(old, s.max(axis=0, keepdims=True))
            top_s[i] = top
            weights.append(jnp.exp2((s - top) * e).astype(jnp.bfloat16))
            keeps.append(jnp.exp2((old - top) * e))
        values = jnp.concatenate([v_r[kb], ones], axis=0)
        for i, p, keep in zip(at, weights, keeps):
            acc[i] = acc[i] * keep + _dot(values, p, 1, 0)

    def attend(kb, g):
        first = g * 8 + side * 4

        @pl.when(kb < first)
        def _():
            block(kb, g, False)

        @pl.when((kb >= first) & (kb < first + 4))
        def _():
            block(kb, g, True)

    def finish(n, _):
        m = lax.rem(n, 4)
        i = n - m + lax.rem(m + 2 - 2 * lax.rem(z, 2), 4)
        o_s[i] = (acc[i, :HEAD, :] * (1 / acc[i, HEAD : HEAD + 1, :])).T.astype(jnp.bfloat16)
        to = lax.div(i, 4) * 8 + side * 4 + lax.rem(i, 4)
        j = head * 2 + core
        deliver(o_s.at[i], o_r.at[j], o_send.at[i], o_recv.at[j], to)

    def place_of(m):
        return jnp.where((side == 1) & (m >= 1) & (m <= 3), 1 + lax.rem(m, 3), m)

    def row_of(m):
        return jnp.where(lax.rem(place_of(m), 2) == 0, y, 1 - y)

    def chip_at(m):
        pair = lax.div(place_of(m), 2)
        across = 4 * side + 1 - z
        near, far = 2 - side, 3 - 3 * side
        second_column, third_column = jnp.where(side == 1, near, across), jnp.where(side == 1, across, near)
        column = jnp.where(pair == 0, z, jnp.where(pair == 1, second_column, jnp.where(pair == 2, third_column, far)))
        return row_of(m) * 8 + column * 2

    def chip(m, _):
        base = chip_at(m)

        @pl.when((side == 1) | (base < 12))
        def _():
            mine, other = base + core, base + 1 - core
            arrived(k_r.at[mine], k_recv.at[mine])
            arrived(v_r.at[mine], v_recv.at[mine])
            sibling = me + 1 - 2 * core
            for ref, send, recv in ((k_r, kf_send, k_recv), (v_r, vf_send, v_recv)):
                pltpu.make_async_remote_copy(src_ref=ref.at[mine], dst_ref=ref.at[mine], send_sem=send.at[m], recv_sem=recv.at[mine],
                                             device_id=(dp, sibling), device_id_type=pl.DeviceIdType.MESH).start()
            last = (side == 1) & (m == 7)

            def part(i, _):
                half = jnp.where(last, lax.rem(i, 2), lax.div(i, 2))
                g = jnp.where(last, lax.div(i, 2), lax.rem(i, 2))

                @pl.when(i == jnp.where(last, 1, 2))
                def _():
                    arrived(k_r.at[other], k_recv.at[other])
                    arrived(v_r.at[other], v_recv.at[other])

                attend(jnp.where(half == 0, mine, other), g)

                @pl.when(last & (i == 1) & (row_of(m) == 0))
                def _():
                    lax.fori_loop(0, 4, finish, None)

            lax.fori_loop(0, 4, part, None)

        @pl.when(m == jnp.where(side == 0, 3, jnp.where(y == 0, 6, 8)))
        def _():
            lax.fori_loop(0, 4, finish, None)

        @pl.when(m == 7)
        def _():
            lax.fori_loop(4, 8, finish, None)

    lax.fori_loop(0, 8, chip, None)

    for i in range(4):
        j = (lax.rem(y + i % 2, 2) * 2 + lax.rem(lax.rem(z, 2) + i // 2, 2)) * 2
        for n in range(2):
            arrived(o_s.at[0], o_recv.at[j + n])

        def columns(n, _):
            at = pl.ds(pl.multiple_of(n * HEAD, HEAD), HEAD)
            if i == 0:
                out_weights(n).wait()
            w = wq_s[pl.ds(pl.multiple_of(n * width + j * HEAD, 2 * HEAD), 2 * HEAD), :]
            part = _dot(o_r[j], w[:HEAD], 1, 0) + _dot(o_r[j + 1], w[HEAD:], 1, 0)
            part += x_ref[:, at].astype(jnp.float32) if i == 0 else y_s[:, at]
            if i < 3:
                y_s[:, at] = part
            else:
                y_ref[:, at] = part.astype(jnp.bfloat16)

        lax.fori_loop(0, d // HEAD, columns, None)

    def left(ref, sem):
        pltpu.make_async_copy(ref, ref, sem).wait()

    def ends(n, _):
        for s in range(2):
            @pl.when((kv_to(n, s) != me) & ((s == side) | (side == 0) | (me < 12)))
            def _():
                left(k_own.at[n], k_send.at[n * 2 + s])
                left(v_own.at[n], v_send.at[n * 2 + s])

    lax.fori_loop(0, KV, ends, None)

    def q_ends(n, _):
        @pl.when(q_to(n) != me)
        def _():
            left(q_own.at[n], q_send.at[n])

        @pl.when(n != slot)
        def _():
            left(o_s.at[n], o_send.at[n])


    lax.fori_loop(0, HEADS, q_ends, None)

    def f_ends(m, _):
        base = chip_at(m)

        @pl.when((side == 1) | (base < 12))
        def _():
            left(k_r.at[0], kf_send.at[m])
            left(v_r.at[0], vf_send.at[m])

    lax.fori_loop(0, 8, f_ends, None)


def solution(mesh):
    def step(x, gain, wq, wk, wv, wo):
        t, d = x.shape
        half = HEAD // 2
        power = float(THETA) ** (-np.arange(half) / half)
        turns = [np.concatenate([np.cos(a), np.sin(a)], 1).astype(np.float32) for a in (np.arange(t)[:, None] * power,
                                                                                      np.arange(DEVICES)[:, None] * t * power)]
        turns[1] = np.repeat(turns[1][:, None], 8, 1)
        bf, f32, dma = jnp.bfloat16, jnp.float32, pltpu.SemaphoreType.DMA
        vmem, hbm = pl.BlockSpec(memory_space=pltpu.VMEM), pl.BlockSpec(memory_space=pl.ANY)
        return pl.pallas_call(
            _kernel,
            in_specs=[vmem] * 4 + [hbm] * 4,
            out_specs=vmem,
            out_shape=jax.ShapeDtypeStruct((t, d), bf),
            scratch_shapes=[
                pltpu.VMEM((t, d), bf), pltpu.VMEM((t, half), f32), pltpu.VMEM((t, half), f32),
                pltpu.VMEM((KV, d, HEAD), bf), pltpu.VMEM((KV, d, HEAD), bf), pltpu.VMEM((HEADS * d, HEAD), bf),
                pltpu.VMEM((KV, t, HEAD), bf), pltpu.VMEM((KV, HEAD, t), bf), pltpu.VMEM((HEADS, t, HEAD), bf),
                pltpu.VMEM((DEVICES, t, HEAD), bf), pltpu.VMEM((DEVICES, HEAD, t), bf), pltpu.VMEM((8, t, HEAD), bf),
                pltpu.VMEM((8, HEAD + 8, t), f32), pltpu.VMEM((8, 1, t), f32), pltpu.VMEM((8, t, HEAD), bf),
                pltpu.VMEM((HEADS, t, HEAD), bf), pltpu.VMEM((t, d), f32),
                dma((2 * KV + HEADS,)), dma((d // HEAD,)), dma((2 * KV,)), dma((2 * KV,)), dma((HEADS,)), dma((8,)), dma((8,)), dma((8,)),
                dma((DEVICES,)), dma((DEVICES,)), dma((8,)), dma((HEADS,)),
            ],
            compiler_params=pltpu.CompilerParams(has_side_effects=True, collective_id=0, vmem_limit_bytes=VMEM),
            name="attention",
        )(x, gain, *turns, wk, wv, wq, wo)

    tokens, whole = P(("dp", "sp"), None), P(None, None)
    return jax.shard_map(
        step,
        mesh=mesh,
        in_specs=(tokens, P(None), whole, whole, whole, whole),
        out_specs=tokens,
        check_vma=False,
    )
```
